32 devices in a mesh: seq: 16 (over z, x, core), head: 2 (over y).
Axes of the slice: x: 2, y: 2, z: 4, core: 2. Of those that a mesh axis runs over, the one named last changes fastest.
Arguments:
- query_rows: bfloat16 [3072, 2048], P('seq', 'head'), may hold values from -6 to 6
- key_rows: bfloat16 [3072, 2048], P('seq', 'head'), may hold values from -6 to 6
- value_rows: bfloat16 [3072, 2048], P('seq', 'head'), may hold values from -6 to 6
- grad_output: bfloat16 [3072, 2048], P('seq', 'head'), may hold values from -6 to 6
- positions: int32 [3072], P('seq'), may hold values from 0 to 3071, each once
Outputs:
- grad_query: bfloat16 [3072, 2048], P(('seq', 'head'))
- grad_keys: bfloat16 [3072, 2048], P('seq', 'head')
- grad_values: bfloat16 [3072, 2048], P('seq', 'head')
The draws below stay inside these ranges and needn't reach their ends.
Inputs may be any that keep to these rules, and one draw needn't show every extreme that they name: `positions`: each number from 0 to 3071 appears once.
All inputs are finite; a program needn't handle non-finite values.
Results may differ from the reference program's by a relative error of at most 0.012.
Values may be sent and summed in bfloat16 or wider, within the bound.
A program may use at most 128 MiB of HBM per device.

```python
import jax
import jax.numpy as jnp
from jax import lax

HEADS = 16
HEAD_DIM = 128
TOKENS = 3072


def base_rows(key, salt):
    noise_key = jax.random.fold_in(jax.random.fold_in(key, salt), 0)
    drawn = jax.random.normal(noise_key, (TOKENS, HEADS * HEAD_DIM), jnp.float32)
    return jnp.clip(drawn, -6.0, 6.0)


def draw_query_rows(key, part):
    drawn = base_rows(key, 1)
    return drawn.astype(jnp.bfloat16)


def draw_key_rows(key, part):
    drawn = base_rows(key, 2)
    return drawn.astype(jnp.bfloat16)


def block_levels(rng, shape, shards, smallest, high):
    def one(position, parts):
        heights = jax.random.uniform(jax.random.fold_in(jax.random.fold_in(rng, 6), position), (parts,), jnp.float32, smallest / len(shards), high / len(shards))
        return jnp.repeat(jnp.exp(heights), shape[position] // parts).reshape((-1,) + (1,) * (len(shape) - position - 1))

    factor_of = one(*shards[0])
    for cut in shards[1:]:
        factor_of = factor_of * one(*cut)
    return factor_of


def scatter_about(rng, extent, spread, most, cuts=(), held_as=jnp.bfloat16):
    entries = jax.random.normal(rng, extent, jnp.float32) * spread
    if len(cuts) > 0:
        entries = block_levels(rng, extent, cuts, -0.22, 0.18) * entries
    return jnp.clip(entries, min=-most, max=most).astype(held_as)


def setup_inputs(seed: int = 0) -> dict:
    streams_of = jax.random.split(jax.random.key(seed), 6)
    return {
        "query_rows": draw_query_rows(jax.random.fold_in(streams_of[5], 71), 0),
        "key_rows": draw_key_rows(jax.random.fold_in(streams_of[5], 71), 0),
        "value_rows": scatter_about(streams_of[2], (TOKENS, HEADS * HEAD_DIM), 1.0, 6.0, ((0, 16), (1, 2))),
        "grad_output": scatter_about(streams_of[3], (TOKENS, HEADS * HEAD_DIM), 1.0, 6.0, ((0, 16), (1, 2))),
        "positions": jax.random.permutation(streams_of[4], TOKENS).astype(jnp.int32),
    }


def reference(query_rows, key_rows, value_rows, grad_output, positions):
    tokens = query_rows.shape[0]
    scaling = HEAD_DIM ** -0.5
    allowed = positions[None, :] <= positions[:, None]

    def per_head(matrix):
        return jnp.swapaxes(matrix.reshape(tokens, HEADS, HEAD_DIM), 0, 1)

    def back_rows(matrix):
        return jnp.swapaxes(matrix, 0, 1).reshape(tokens, HEADS * HEAD_DIM)

    def one_head(head_items):
        query_full = head_items[0].astype(jnp.float32)
        key_full = head_items[1].astype(jnp.float32)
        value_full = head_items[2].astype(jnp.float32)
        grad_full = head_items[3].astype(jnp.float32)
        highest = lax.Precision.HIGHEST
        scores = jnp.dot(query_full, key_full.T, precision=highest) * scaling
        masked = jnp.where(allowed, scores, -1.0e30)
        top_score = jnp.max(masked, axis=1)
        denominator = jnp.sum(jnp.where(allowed, jnp.exp(masked - top_score[:, None]), 0.0), axis=1)
        log_total = top_score + jnp.log(denominator)
        probabilities = jnp.where(allowed, jnp.exp(masked - log_total[:, None]), 0.0)
        weights = probabilities.astype(jnp.bfloat16).astype(jnp.float32)
        grad_probs = jnp.dot(grad_full, value_full.T, precision=highest)
        row_delta = jnp.sum(probabilities * grad_probs, axis=1)
        grad_value = jnp.dot(weights.T, grad_full, precision=highest)
        grad_scores = (probabilities * (grad_probs - row_delta[:, None]) * scaling).astype(jnp.bfloat16).astype(jnp.float32)
        grad_query = jnp.dot(grad_scores, key_full, precision=highest)
        grad_key = jnp.dot(grad_scores.T, query_full, precision=highest)
        return grad_query.astype(jnp.bfloat16), grad_key.astype(jnp.bfloat16), grad_value.astype(jnp.bfloat16)

    grad_query, grad_keys, grad_values = lax.map(one_head, (per_head(query_rows), per_head(key_rows), per_head(value_rows), per_head(grad_output)))
    return back_rows(grad_query), back_rows(grad_keys), back_rows(grad_values)
```

```python
import functools

import jax
import jax.numpy as jnp
from jax import lax
from jax.experimental import pallas as pl
from jax.experimental.pallas import tpu as pltpu
from jax.sharding import PartitionSpec as P

HEAD_DIM = 128
MESH = pl.DeviceIdType.MESH
NT = (((1,), (1,)), ((), ()))
TN = (((0,), (0,)), ((), ()))


def kernel(
    members, heads, groups, rows, width,
    pos_ref, q_hbm, k_hbm, v_hbm, g_hbm,
    dq_out, dk_out, dv_out,
    q_buf, g_buf, k_buf, v_buf, pos_buf, key_pos, query_pos,
    z_buf, p_buf, dk_acc, dv_acc, dq_acc, kv_stage, kv_mates, kv_final, kv_back, dq_stage, dq_back,
    local_sem, in_send, in_recv, pos_send, pos_recv, mate_send, mate_recv,
    part_send, part_recv, back_send, back_recv, dq_send, dq_recv,
):
    ratio = members // heads
    me = lax.axis_index("seq")
    group = lax.axis_index("head")
    mine = me // ratio
    lane = lax.rem(me, ratio)
    scaling = HEAD_DIM ** (-0.5)

    barrier = pltpu.get_barrier_semaphore()
    for d in range(1, members):
        pl.semaphore_signal(
            barrier, inc=1,
            device_id={"seq": lax.rem(me + d, members), "head": group}, device_id_type=MESH,
        )
    for e in range(1, groups):
        for j in range(heads):
            pl.semaphore_signal(
                barrier, inc=1,
                device_id={
                    "seq": lax.rem(mine + j, heads) * ratio + lane,
                    "head": lax.rem(group + e, groups),
                },
                device_id_type=MESH,
            )
    pl.semaphore_wait(barrier, members - 1 + (groups - 1) * heads)

    def columns(index):
        return pl.ds(pl.multiple_of(index * HEAD_DIM, HEAD_DIM), HEAD_DIM)

    my_slot = lane * heads + mine
    pairs = (
        (k_hbm, k_buf, my_slot), (v_hbm, v_buf, my_slot), (q_hbm, q_buf, mine), (g_hbm, g_buf, mine)
    )
    pos_copies = []
    for d in range(1, members):
        copy = pltpu.make_async_remote_copy(
            src_ref=pos_ref, dst_ref=pos_buf.at[my_slot],
            send_sem=pos_send.at[d], recv_sem=pos_recv.at[d],
            device_id={"seq": lax.rem(me + d, members), "head": group}, device_id_type=MESH,
        )
        copy.start()
        pos_copies.append(copy)
    arrivals = [[] for _ in range(heads)]
    for a, (source, target, slot) in enumerate(pairs):
        copy = pltpu.make_async_copy(
            source.at[:, columns(mine)], target.at[slot], local_sem.at[a]
        )
        copy.start()
        arrivals[0].append(copy)
    for j in range(1, heads):
        other = lax.rem(mine + j, heads)
        for a, (source, target, slot) in enumerate(pairs):
            copy = pltpu.make_async_remote_copy(
                src_ref=source.at[:, columns(other)], dst_ref=target.at[slot],
                send_sem=in_send.at[a, j], recv_sem=in_recv.at[a, j],
                device_id={"seq": other * ratio + lane, "head": group}, device_id_type=MESH,
            )
            copy.start()
            arrivals[j].append(copy)

    mate_copies = []

    def forward(j):
        slot = lane * heads + lax.rem(mine + heads - j, heads)
        for a, buf in enumerate((k_buf, v_buf)):
            for m in range(1, ratio):
                copy = pltpu.make_async_remote_copy(
                    src_ref=buf.at[slot], dst_ref=buf.at[slot],
                    send_sem=mate_send.at[a, m, j], recv_sem=mate_recv.at[a, m, j],
                    device_id={"seq": mine * ratio + lax.rem(lane + m, ratio), "head": group},
                    device_id_type=MESH,
                )
                copy.start()
                mate_copies.append(copy)

    for j in range(heads):
        for a in range(2):
            arrivals[j][a].wait()
        forward(j)

    for copy in pos_copies:
        copy.wait()
    pos_buf[my_slot] = pos_ref[...]

    def spread(slot, carry):
        row = jnp.broadcast_to(pos_buf[slot][0:1, :], (HEAD_DIM, width))
        key_pos[slot] = row.T[:rows]
        return carry

    lax.fori_loop(0, members, spread, 0)
    for j in range(heads):
        for a in range(2, 4):
            arrivals[j][a].wait()
    for copy in mate_copies:
        copy.wait()

    per_block = q_buf.shape[0] if heads % 4 else 4
    blocks = heads // per_block
    block = per_block * rows
    part_rows = rows // groups

    dq_copies = []
    for b in range(blocks):
        sources = [
            lax.rem(mine + heads - (b * per_block + x), heads) for x in range(per_block)
        ]
        query = jnp.concatenate([q_buf[i] for i in sources], axis=0)
        grad = jnp.concatenate([g_buf[i] for i in sources], axis=0)
        for x, i in enumerate(sources):
            query_pos[x * rows:(x + 1) * rows, :] = key_pos[lane * heads + i]
        pos_row = query_pos[...].T[0:1, :]

        def scores_turn(slot, top):
            scores = lax.dot_general(k_buf[slot], query, NT, preferred_element_type=jnp.float32)
            held = jnp.concatenate([key_pos[slot]] * (block // HEAD_DIM), axis=1)
            scores = jnp.where(held <= pos_row, scores * scaling, -1e30)
            z_buf[slot] = scores
            return jnp.maximum(top, jnp.max(scores.reshape(rows // 8, 8, block), axis=0))

        top = lax.fori_loop(
            0, members, scores_turn, jnp.full((8, block), -1e30, jnp.float32)
        )
        top = jnp.max(top, axis=0, keepdims=True)

        def stats_turn(slot, carry):
            total, delta = carry
            unscaled = jnp.exp(z_buf[slot] - top)
            probs = lax.dot_general(v_buf[slot], grad, NT, preferred_element_type=jnp.float32)
            z_buf[slot] = unscaled
            p_buf[slot] = probs
            total = total + jnp.sum(unscaled.reshape(rows // 8, 8, block), axis=0)
            delta = delta + jnp.sum((unscaled * probs).reshape(rows // 8, 8, block), axis=0)
            return total, delta

        zero = jnp.zeros((8, block), jnp.float32)
        total, delta = lax.fori_loop(0, members, stats_turn, (zero, zero))
        inverse = 1.0 / jnp.sum(total, axis=0, keepdims=True)
        delta = jnp.sum(delta, axis=0, keepdims=True) * inverse

        dq_acc[...] = jnp.zeros_like(dq_acc)

        def terms(slot):
            weights = z_buf[slot] * inverse
            value_term = jnp.dot(
                weights.astype(jnp.bfloat16), grad, preferred_element_type=jnp.float32
            )
            grad_scores = (weights * ((p_buf[slot] - delta) * scaling)).astype(jnp.bfloat16)
            key_term = jnp.dot(grad_scores, query, preferred_element_type=jnp.float32)
            dq_acc[...] += lax.dot_general(
                k_buf[slot], grad_scores, TN, preferred_element_type=jnp.float32
            )
            if b > 0:
                key_term = key_term + dk_acc[slot]
                value_term = value_term + dv_acc[slot]
            return key_term, value_term

        if b < blocks - 1:

            def grads_turn(slot, carry):
                key_term, value_term = terms(slot)
                dk_acc[slot] = key_term
                dv_acc[slot] = value_term
                return carry

            lax.fori_loop(0, members, grads_turn, 0)
        else:
            def part_copy(m, i):
                other = lax.rem(lane + m, ratio)
                return pltpu.make_async_remote_copy(
                    src_ref=kv_stage.at[m - 1, i], dst_ref=kv_mates.at[m - 1, i],
                    send_sem=part_send.at[m, i], recv_sem=part_recv.at[m, i],
                    device_id={"seq": mine * ratio + other, "head": group}, device_id_type=MESH,
                )

            for m in range(1, ratio):

                def mate_turn(j, carry):
                    i = lax.rem(mine + 1 + j, heads)
                    slot = lax.rem(lane + m, ratio) * heads + i
                    key_term, value_term = terms(slot)
                    kv_stage[m - 1, i, 0] = key_term.astype(jnp.bfloat16)
                    kv_stage[m - 1, i, 1] = value_term.astype(jnp.bfloat16)
                    part_copy(m, i).start()
                    return carry

                lax.fori_loop(0, heads, mate_turn, 0)

            def back_copy(j):
                i = lax.rem(mine + 1 + j, heads)
                return pltpu.make_async_remote_copy(
                    src_ref=kv_final.at[i], dst_ref=kv_back.at[mine],
                    send_sem=back_send.at[j], recv_sem=back_recv.at[j],
                    device_id={"seq": i * ratio + lane, "head": group}, device_id_type=MESH,
                )

            def own_turn(j):
                i = lax.rem(mine + 1 + j, heads)
                key_term, value_term = terms(lane * heads + i)
                for m in range(1, ratio):
                    part_copy(m, i).wait()
                    key_term = key_term + kv_mates[m - 1, i, 0].astype(jnp.float32)
                    value_term = value_term + kv_mates[m - 1, i, 1].astype(jnp.float32)
                return i, key_term.astype(jnp.bfloat16), value_term.astype(jnp.bfloat16)

            def own_step(j, carry):
                i, key_term, value_term = own_turn(j)
                kv_final[i, 0] = key_term
                kv_final[i, 1] = value_term
                back_copy(j).start()
                return carry

            lax.fori_loop(0, heads - 1, own_step, 0)
            i, key_term, value_term = own_turn(heads - 1)
            kv_back[i, 0] = key_term
            kv_back[i, 1] = value_term

        grad_query = dq_acc[...].T
        for x, i in enumerate(sources):
            j = b * per_block + x
            for e in range(groups):
                other = lax.rem(group + e, groups)
                for r in range(groups):
                    if e == 0:
                        start = x * rows + r * part_rows
                        dq_stage[j, r] = grad_query[start:start + part_rows].astype(jnp.bfloat16)
            for e in range(groups):
                other = lax.rem(group + e, groups)
                if j == 0 and e == 0:
                    dq_back[group * heads + mine] = dq_stage[j, group]
                    continue
                copy = pltpu.make_async_remote_copy(
                    src_ref=dq_stage.at[j, other], dst_ref=dq_back.at[group * heads + mine],
                    send_sem=dq_send.at[j, e], recv_sem=dq_recv.at[j, e],
                    device_id={"seq": i * ratio + lane, "head": other}, device_id_type=MESH,
                )
                copy.start()
                dq_copies.append(copy)

    for j in range(heads - 1):
        back_copy(j).wait()
    for h in range(heads):
        dk_out[:, h * HEAD_DIM:(h + 1) * HEAD_DIM] = kv_back[h, 0]
        dv_out[:, h * HEAD_DIM:(h + 1) * HEAD_DIM] = kv_back[h, 1]
    for copy in dq_copies:
        copy.wait()
    for h in range(groups * heads):
        dq_out[:, h * HEAD_DIM:(h + 1) * HEAD_DIM] = dq_back[h]


def local(members, groups, query_rows, key_rows, value_rows, grad_output, positions):
    rows, wide = query_rows.shape
    heads = wide // HEAD_DIM
    ratio = members // heads
    width = -(-rows // HEAD_DIM) * HEAD_DIM
    per_block = heads if heads % 4 else 4
    block = per_block * rows
    position_rows = jnp.broadcast_to(
        jnp.pad(positions.astype(jnp.float32), (0, width - rows))[None], (8, width)
    )
    low, full = jnp.bfloat16, jnp.float32
    piece = (rows, HEAD_DIM)
    dma = pltpu.SemaphoreType.DMA
    scratch = [
        pltpu.VMEM((heads,) + piece, low),
        pltpu.VMEM((heads,) + piece, low),
        pltpu.VMEM((members,) + piece, low),
        pltpu.VMEM((members,) + piece, low),
        pltpu.VMEM((members, 8, width), full),
        pltpu.VMEM((members,) + piece, full),
        pltpu.VMEM((block, HEAD_DIM), full),
        pltpu.VMEM((members, rows, block), full),
        pltpu.VMEM((members, rows, block), full),
        pltpu.VMEM((members,) + piece, full),
        pltpu.VMEM((members,) + piece, full),
        pltpu.VMEM((HEAD_DIM, block), full),
        pltpu.VMEM((max(ratio - 1, 1), heads, 2) + piece, low),
        pltpu.VMEM((max(ratio - 1, 1), heads, 2) + piece, low),
        pltpu.VMEM((heads, 2) + piece, low),
        pltpu.VMEM((heads, 2) + piece, low),
        pltpu.VMEM((heads, groups, rows // groups, HEAD_DIM), low),
        pltpu.VMEM((groups * heads, rows // groups, HEAD_DIM), low),
        dma((4,)), dma((4, heads)), dma((4, heads)), dma((members,)), dma((members,)),
        dma((2, ratio, heads)), dma((2, ratio, heads)),
        dma((ratio, heads)), dma((ratio, heads)), dma((heads,)), dma((heads,)),
        dma((heads, groups)), dma((heads, groups)),
    ]
    vmem = pl.BlockSpec(memory_space=pltpu.VMEM)
    hbm = pl.BlockSpec(memory_space=pl.ANY)
    return pl.pallas_call(
        functools.partial(kernel, members, heads, groups, rows, width),
        out_shape=(
            jax.ShapeDtypeStruct((rows // groups, groups * wide), low),
            jax.ShapeDtypeStruct((rows, wide), low),
            jax.ShapeDtypeStruct((rows, wide), low),
        ),
        in_specs=[vmem, hbm, hbm, hbm, hbm],
        out_specs=(vmem, vmem, vmem),
        scratch_shapes=scratch,
        compiler_params=pltpu.CompilerParams(
            collective_id=0, has_side_effects=True, vmem_limit_bytes=60 * 1024 * 1024
        ),
    )(position_rows, query_rows, key_rows, value_rows, grad_output)


def solution(mesh):
    placed = (P("seq", "head"), P("seq", "head"), P("seq", "head"), P("seq", "head"), P("seq"))
    return jax.shard_map(
        functools.partial(local, mesh.shape["seq"], mesh.shape["head"]),
        mesh=mesh,
        in_specs=placed,
        out_specs=(P(("seq", "head"), None), P("seq", "head"), P("seq", "head")),
        check_vma=False,
    )
```

```python
import functools

import jax
import jax.numpy as jnp
from jax import lax
from jax.experimental import pallas as pl
from jax.experimental.pallas import tpu as pltpu
from jax.sharding import PartitionSpec as P

HEAD_DIM = 128
MESH = pl.DeviceIdType.MESH
NT = (((1,), (1,)), ((), ()))
TN = (((0,), (0,)), ((), ()))


def kernel(
    members, heads, groups, rows, width,
    pos_ref, q_hbm, k_hbm, v_hbm, g_hbm,
    dq_out, dk_out, dv_out,
    qg_buf, kv_buf, qg_stage, kv_stage, pos_buf, key_pos, tops,
    z_buf, p_buf, dq_acc, part_stage, part_mates, kv_final, kv_back, dq_stage, dq_back,
    qg_local, kv_local, qg_send, qg_recv, kv_send, kv_recv, pos_send, pos_recv,
    mate_send, mate_recv, part_send, part_recv, back_send, back_recv, dq_send, dq_recv,
):
    ratio = members // heads
    me = lax.axis_index("seq")
    group = lax.axis_index("head")
    mine = me // ratio
    lane = lax.rem(me, ratio)
    scaling = HEAD_DIM ** (-0.5)
    block = heads * rows
    part_rows = rows // groups
    my_slot = lane * heads + mine

    def columns(index):
        return pl.ds(pl.multiple_of(index * HEAD_DIM, HEAD_DIM), HEAD_DIM)

    def local_copies(arrays, stage, first, sems, j):
        other = lax.rem(mine + j, heads)
        return [
            pltpu.make_async_copy(
                array.at[:, columns(other)],
                first.at[a] if j == 0 else stage.at[j, a],
                sems.at[a, j],
            )
            for a, array in enumerate(arrays)
        ]

    qg_locals = [
        local_copies((q_hbm, g_hbm), qg_stage, qg_buf.at[mine], qg_local, j) for j in range(heads)
    ]
    kv_locals = [
        local_copies((k_hbm, v_hbm), kv_stage, kv_buf.at[my_slot], kv_local, j)
        for j in range(heads)
    ]
    for copies in qg_locals[1:] + kv_locals[1:] + qg_locals[:1] + kv_locals[:1]:
        for copy in copies:
            copy.start()

    barrier = pltpu.get_barrier_semaphore()
    for d in range(1, members):
        pl.semaphore_signal(
            barrier, inc=1,
            device_id={"seq": lax.rem(me + d, members), "head": group}, device_id_type=MESH,
        )
    for e in range(1, groups):
        for j in range(heads):
            pl.semaphore_signal(
                barrier, inc=1,
                device_id={
                    "seq": lax.rem(mine + j, heads) * ratio + lane,
                    "head": lax.rem(group + e, groups),
                },
                device_id_type=MESH,
            )
    pl.semaphore_wait(barrier, members - 1 + (groups - 1) * heads)

    def qg_copy(j):
        return pltpu.make_async_remote_copy(
            src_ref=qg_stage.at[j], dst_ref=qg_buf.at[mine],
            send_sem=qg_send.at[j], recv_sem=qg_recv.at[j],
            device_id={"seq": lax.rem(mine + j, heads) * ratio + lane, "head": group},
            device_id_type=MESH,
        )

    def kv_copy(j):
        return pltpu.make_async_remote_copy(
            src_ref=kv_stage.at[j], dst_ref=kv_buf.at[my_slot],
            send_sem=kv_send.at[j], recv_sem=kv_recv.at[j],
            device_id={"seq": lax.rem(mine + j, heads) * ratio + lane, "head": group},
            device_id_type=MESH,
        )

    def pos_copy(d):
        return pltpu.make_async_remote_copy(
            src_ref=pos_ref, dst_ref=pos_buf.at[my_slot],
            send_sem=pos_send.at[d], recv_sem=pos_recv.at[d],
            device_id={"seq": lax.rem(me + d, members), "head": group}, device_id_type=MESH,
        )

    for d in range(1, members):
        pos_copy(d).start()
    for j in range(1, heads):
        for copy in qg_locals[j]:
            copy.wait()
        qg_copy(j).start()
    for j in range(1, heads):
        for copy in kv_locals[j]:
            copy.wait()
        kv_copy(j).start()

    def mate_copy(m, j):
        slot = lane * heads + lax.rem(mine + heads - j, heads)
        return pltpu.make_async_remote_copy(
            src_ref=kv_buf.at[slot], dst_ref=kv_buf.at[slot],
            send_sem=mate_send.at[m, j], recv_sem=mate_recv.at[m, j],
            device_id={"seq": mine * ratio + lax.rem(lane + m, ratio), "head": group},
            device_id_type=MESH,
        )

    pos_buf[my_slot] = pos_ref[...]
    for d in range(1, members):
        pos_copy(d).wait()

    def spread(slot, carry):
        row = jnp.broadcast_to(pos_buf[slot][0:1, :], (HEAD_DIM, width))
        key_pos[slot] = row.T[:rows]
        return carry

    lax.fori_loop(0, members, spread, 0)
    held = key_pos[pl.ds(lane * heads, heads)].reshape(block, HEAD_DIM)
    pos_row = held.T[0:1, :]
    for copy in qg_locals[0] + kv_locals[0]:
        copy.wait()
    for j in range(1, heads):
        qg_copy(j).wait()

    def eights(values):
        return values.reshape(rows // 8, 8, block)

    def stats(slot, carry):
        top, total, delta = carry
        query = qg_buf[:, 0].reshape(block, HEAD_DIM)
        grad = qg_buf[:, 1].reshape(block, HEAD_DIM)
        scores = lax.dot_general(kv_buf[slot, 0], query, NT, preferred_element_type=jnp.float32)
        key_held = jnp.concatenate([key_pos[slot]] * (block // HEAD_DIM), axis=1)
        scores = jnp.where(key_held <= pos_row, scores * scaling, -1e30)
        here = jnp.max(jnp.max(eights(scores), axis=0), axis=0, keepdims=True)
        new_top = jnp.maximum(top, here)
        unscaled = jnp.exp(scores - new_top)
        probs = lax.dot_general(kv_buf[slot, 1], grad, NT, preferred_element_type=jnp.float32)
        z_buf[slot] = unscaled
        p_buf[slot] = probs
        tops[slot] = jnp.broadcast_to(new_top, (8, block))
        alpha = jnp.exp(top - new_top)
        total = total * alpha + jnp.sum(eights(unscaled), axis=0)
        delta = delta * alpha + jnp.sum(eights(unscaled * probs), axis=0)
        return new_top, total, delta

    def arrive_turn(j, carry):
        i = lax.rem(mine + heads - j, heads)

        @pl.when(j > 0)
        def _():
            kv_copy(j).wait()

        def start_turn(m, inner):
            mate_copy(m, j).start()
            return inner

        lax.fori_loop(1, ratio, start_turn, 0)
        carry = stats(lane * heads + i, carry)

        def mate_turn(m, inner):
            mate_copy(m, j).wait()
            return stats(lax.rem(lane + ratio - m, ratio) * heads + i, inner)

        return lax.fori_loop(1, ratio, mate_turn, carry)

    zero = jnp.zeros((8, block), jnp.float32)
    top, total, delta = lax.fori_loop(
        0, heads, arrive_turn, (jnp.full((1, block), -1e30, jnp.float32), zero, zero)
    )
    inverse = 1.0 / jnp.sum(total, axis=0, keepdims=True)
    delta = jnp.sum(delta, axis=0, keepdims=True) * inverse
    dq_acc[...] = jnp.zeros_like(dq_acc)

    def terms(slot):
        query = qg_buf[:, 0].reshape(block, HEAD_DIM)
        grad = qg_buf[:, 1].reshape(block, HEAD_DIM)
        weights = z_buf[slot] * (jnp.exp(tops[slot][0:1] - top) * inverse)
        value_term = jnp.dot(
            weights.astype(jnp.bfloat16), grad, preferred_element_type=jnp.float32
        )
        grad_scores = (weights * ((p_buf[slot] - delta) * scaling)).astype(jnp.bfloat16)
        key_term = jnp.dot(grad_scores, query, preferred_element_type=jnp.float32)
        dq_acc[...] += lax.dot_general(
            kv_buf[slot, 0], grad_scores, TN, preferred_element_type=jnp.float32
        )
        return key_term, value_term

    def part_copy(m, i):
        return pltpu.make_async_remote_copy(
            src_ref=part_stage.at[m - 1, i], dst_ref=part_mates.at[m - 1, i],
            send_sem=part_send.at[m, i], recv_sem=part_recv.at[m, i],
            device_id={"seq": mine * ratio + lax.rem(lane + m, ratio), "head": group},
            device_id_type=MESH,
        )

    def mate_parts(m, carry):
        def mate_part(j, inner):
            i = lax.rem(mine + 1 + j, heads)
            key_term, value_term = terms(lax.rem(lane + m, ratio) * heads + i)
            part_stage[m - 1, i, 0] = key_term.astype(jnp.bfloat16)
            part_stage[m - 1, i, 1] = value_term.astype(jnp.bfloat16)
            part_copy(m, i).start()
            return inner

        return lax.fori_loop(0, heads, mate_part, carry)

    lax.fori_loop(1, ratio, mate_parts, 0)

    def back_copy(j):
        i = lax.rem(mine + 1 + j, heads)
        return pltpu.make_async_remote_copy(
            src_ref=kv_final.at[i], dst_ref=kv_back.at[mine],
            send_sem=back_send.at[j], recv_sem=back_recv.at[j],
            device_id={"seq": i * ratio + lane, "head": group}, device_id_type=MESH,
        )

    def own_step(j, carry):
        i = lax.rem(mine + 1 + j, heads)
        key_term, value_term = terms(lane * heads + i)
        for m in range(1, ratio):
            part_copy(m, i).wait()
            key_term = key_term + part_mates[m - 1, i, 0].astype(jnp.float32)
            value_term = value_term + part_mates[m - 1, i, 1].astype(jnp.float32)
        kv_final[i, 0] = key_term.astype(jnp.bfloat16)
        kv_final[i, 1] = value_term.astype(jnp.bfloat16)

        @pl.when(j < heads - 1)
        def _():
            back_copy(j).start()

        return carry

    lax.fori_loop(0, heads, own_step, 0)
    kv_back[mine] = kv_final[mine]

    grad_query = dq_acc[...].T.astype(jnp.bfloat16)
    dq_stage[...] = grad_query.reshape(heads, groups, part_rows, HEAD_DIM)

    def dq_copy(j, e):
        i = lax.rem(mine + 1 + j, heads)
        other = lax.rem(group + e, groups)
        return pltpu.make_async_remote_copy(
            src_ref=dq_stage.at[i, other], dst_ref=dq_back.at[group * heads + mine],
            send_sem=dq_send.at[j, e], recv_sem=dq_recv.at[j, e],
            device_id={"seq": i * ratio + lane, "head": other}, device_id_type=MESH,
        )

    remote = [(j, e) for j in range(heads) for e in range(groups) if (j, e) != (heads - 1, 0)]
    for j, e in remote:
        dq_copy(j, e).start()
    dq_back[group * heads + mine] = dq_stage[mine, group]

    for j in range(heads - 1):
        back_copy(j).wait()
    for h in range(heads):
        dk_out[:, h * HEAD_DIM:(h + 1) * HEAD_DIM] = kv_back[h, 0]
        dv_out[:, h * HEAD_DIM:(h + 1) * HEAD_DIM] = kv_back[h, 1]
    for j, e in remote:
        dq_copy(j, e).wait()
    for h in range(groups * heads):
        dq_out[:, h * HEAD_DIM:(h + 1) * HEAD_DIM] = dq_back[h]


def local(members, groups, query_rows, key_rows, value_rows, grad_output, positions):
    rows, wide = query_rows.shape
    heads = wide // HEAD_DIM
    ratio = members // heads
    width = -(-rows // HEAD_DIM) * HEAD_DIM
    block = heads * rows
    position_rows = jnp.broadcast_to(
        jnp.pad(positions.astype(jnp.float32), (0, width - rows))[None], (8, width)
    )
    low, full = jnp.bfloat16, jnp.float32
    piece = (rows, HEAD_DIM)
    dma = pltpu.SemaphoreType.DMA
    mates = max(ratio - 1, 1)
    scratch = [
        pltpu.VMEM((heads, 2) + piece, low),
        pltpu.VMEM((members, 2) + piece, low),
        pltpu.VMEM((heads, 2) + piece, low),
        pltpu.VMEM((heads, 2) + piece, low),
        pltpu.VMEM((members, 8, width), full),
        pltpu.VMEM((members,) + piece, full),
        pltpu.VMEM((members, 8, block), full),
        pltpu.VMEM((members, rows, block), full),
        pltpu.VMEM((members, rows, block), full),
        pltpu.VMEM((HEAD_DIM, block), full),
        pltpu.VMEM((mates, heads, 2) + piece, low),
        pltpu.VMEM((mates, heads, 2) + piece, low),
        pltpu.VMEM((heads, 2) + piece, low),
        pltpu.VMEM((heads, 2) + piece, low),
        pltpu.VMEM((heads, groups, rows // groups, HEAD_DIM), low),
        pltpu.VMEM((groups * heads, rows // groups, HEAD_DIM), low),
        dma((2, heads)), dma((2, heads)), dma((heads,)), dma((heads,)), dma((heads,)),
        dma((heads,)), dma((members,)), dma((members,)),
        dma((ratio, heads)), dma((ratio, heads)),
        dma((ratio, heads)), dma((ratio, heads)), dma((heads,)), dma((heads,)),
        dma((heads, groups)), dma((heads, groups)),
    ]
    vmem = pl.BlockSpec(memory_space=pltpu.VMEM)
    hbm = pl.BlockSpec(memory_space=pl.ANY)
    return pl.pallas_call(
        functools.partial(kernel, members, heads, groups, rows, width),
        out_shape=(
            jax.ShapeDtypeStruct((rows // groups, groups * wide), low),
            jax.ShapeDtypeStruct((rows, wide), low),
            jax.ShapeDtypeStruct((rows, wide), low),
        ),
        in_specs=[vmem, hbm, hbm, hbm, hbm],
        out_specs=(vmem, vmem, vmem),
        scratch_shapes=scratch,
        compiler_params=pltpu.CompilerParams(
            collective_id=0, has_side_effects=True, vmem_limit_bytes=63 * 1024 * 1024
        ),
    )(position_rows, query_rows, key_rows, value_rows, grad_output)


def solution(mesh):
    placed = (P("seq", "head"), P("seq", "head"), P("seq", "head"), P("seq", "head"), P("seq"))
    return jax.shard_map(
        functools.partial(local, mesh.shape["seq"], mesh.shape["head"]),
        mesh=mesh,
        in_specs=placed,
        out_specs=(P(("seq", "head"), None), P("seq", "head"), P("seq", "head")),
        check_vma=False,
    )
```

```python
import functools

import jax
import jax.numpy as jnp
from jax import lax
from jax.experimental import pallas as pl
from jax.experimental.pallas import tpu as pltpu
from jax.sharding import PartitionSpec as P

HEAD_DIM = 128
MESH = pl.DeviceIdType.MESH
NT = (((1,), (1,)), ((), ()))
TN = (((0,), (0,)), ((), ()))


def kernel(
    members, heads, groups, rows, width,
    pos_ref, q_hbm, k_hbm, v_hbm, g_hbm,
    dq_out, dk_out, dv_out,
    qg_buf, kv_buf, qg_stage, kv_stage, pos_buf, key_pos, tops,
    z_buf, p_buf, dq_acc, part_stage, part_mates, kv_final, kv_back, dq_stage, dq_back,
    qg_local, kv_local, qg_send, qg_recv, kv_send, kv_recv, pos_send, pos_recv,
    mate_send, mate_recv, part_send, part_recv, back_send, back_recv, dq_send, dq_recv,
):
    ratio = members // heads
    me = lax.axis_index("seq")
    group = lax.axis_index("head")
    mine = me // ratio
    lane = lax.rem(me, ratio)
    scaling = HEAD_DIM ** (-0.5)
    block = heads * rows
    part_rows = rows // groups
    my_slot = lane * heads + mine

    def columns(index):
        return pl.ds(pl.multiple_of(index * HEAD_DIM, HEAD_DIM), HEAD_DIM)

    def local_copies(arrays, stage, first, sems, j):
        other = lax.rem(mine + j, heads)
        return [
            pltpu.make_async_copy(
                array.at[:, columns(other)],
                first.at[a] if j == 0 else stage.at[j, a],
                sems.at[a, j],
            )
            for a, array in enumerate(arrays)
        ]

    qg_locals = [
        local_copies((q_hbm, g_hbm), qg_stage, qg_buf.at[mine], qg_local, j) for j in range(heads)
    ]
    kv_locals = [
        local_copies((k_hbm, v_hbm), kv_stage, kv_buf.at[my_slot], kv_local, j)
        for j in range(heads)
    ]
    for copies in qg_locals[1:] + kv_locals[1:] + qg_locals[:1] + kv_locals[:1]:
        for copy in copies:
            copy.start()

    barrier = pltpu.get_barrier_semaphore()
    for d in range(1, members):
        pl.semaphore_signal(
            barrier, inc=1,
            device_id={"seq": lax.rem(me + d, members), "head": group}, device_id_type=MESH,
        )
    for e in range(1, groups):
        for j in range(heads):
            pl.semaphore_signal(
                barrier, inc=1,
                device_id={
                    "seq": lax.rem(mine + j, heads) * ratio + lane,
                    "head": lax.rem(group + e, groups),
                },
                device_id_type=MESH,
            )
    pl.semaphore_wait(barrier, members - 1 + (groups - 1) * heads)

    def qg_copy(j):
        return pltpu.make_async_remote_copy(
            src_ref=qg_stage.at[j], dst_ref=qg_buf.at[mine],
            send_sem=qg_send.at[j], recv_sem=qg_recv.at[j],
            device_id={"seq": lax.rem(mine + j, heads) * ratio + lane, "head": group},
            device_id_type=MESH,
        )

    def kv_copy(j):
        return pltpu.make_async_remote_copy(
            src_ref=kv_stage.at[j], dst_ref=kv_buf.at[my_slot],
            send_sem=kv_send.at[j], recv_sem=kv_recv.at[j],
            device_id={"seq": lax.rem(mine + j, heads) * ratio + lane, "head": group},
            device_id_type=MESH,
        )

    def pos_copy(d):
        return pltpu.make_async_remote_copy(
            src_ref=pos_ref, dst_ref=pos_buf.at[my_slot],
            send_sem=pos_send.at[d], recv_sem=pos_recv.at[d],
            device_id={"seq": lax.rem(me + d, members), "head": group}, device_id_type=MESH,
        )

    for d in range(1, members):
        pos_copy(d).start()
    for j in range(1, heads):
        for copy in qg_locals[j]:
            copy.wait()
        qg_copy(j).start()
    for j in range(1, heads):
        for copy in kv_locals[j]:
            copy.wait()
        kv_copy(j).start()

    def mate_copy(m, j):
        slot = lane * heads + lax.rem(mine + heads - j, heads)
        return pltpu.make_async_remote_copy(
            src_ref=kv_buf.at[slot], dst_ref=kv_buf.at[slot],
            send_sem=mate_send.at[m, j], recv_sem=mate_recv.at[m, j],
            device_id={"seq": mine * ratio + lax.rem(lane + m, ratio), "head": group},
            device_id_type=MESH,
        )

    pos_buf[my_slot] = pos_ref[...]
    for d in range(1, members):
        pos_copy(d).wait()

    def spread(slot, carry):
        row = jnp.broadcast_to(pos_buf[slot][0:1, :], (HEAD_DIM, width))
        key_pos[slot] = row.T[:rows]
        return carry

    lax.fori_loop(0, members, spread, 0)
    held = key_pos[pl.ds(lane * heads, heads)].reshape(block, HEAD_DIM)
    pos_row = held.T[0:1, :]
    for copy in qg_locals[0] + kv_locals[0]:
        copy.wait()
    for j in range(1, heads):
        qg_copy(j).wait()

    def eights(values):
        return values.reshape(rows // 8, 8, block)

    def stats(slot, carry):
        top, total, delta = carry
        query = qg_buf[:, 0].reshape(block, HEAD_DIM)
        grad = qg_buf[:, 1].reshape(block, HEAD_DIM)
        scores = lax.dot_general(kv_buf[slot, 0], query, NT, preferred_element_type=jnp.float32)
        key_held = jnp.concatenate([key_pos[slot]] * (block // HEAD_DIM), axis=1)
        scores = jnp.where(key_held <= pos_row, scores * scaling, -1e30)
        here = jnp.max(jnp.max(eights(scores), axis=0), axis=0, keepdims=True)
        new_top = jnp.maximum(top, here)
        unscaled = jnp.exp(scores - new_top)
        probs = lax.dot_general(kv_buf[slot, 1], grad, NT, preferred_element_type=jnp.float32)
        z_buf[slot] = unscaled
        p_buf[slot] = probs
        tops[slot] = jnp.broadcast_to(new_top, (8, block))
        alpha = jnp.exp(top - new_top)
        total = total * alpha + jnp.sum(eights(unscaled), axis=0)
        delta = delta * alpha + jnp.sum(eights(unscaled * probs), axis=0)
        return new_top, total, delta

    def arrive_turn(step, carry):
        j = step // ratio
        m = lax.rem(step, ratio)
        i = lax.rem(mine + heads - j, heads)

        @pl.when((m == 0) & (j > 0))
        def _():
            kv_copy(j).wait()

        @pl.when(m == 0)
        def _():
            def start_turn(other, inner):
                mate_copy(other, j).start()
                return inner

            lax.fori_loop(1, ratio, start_turn, 0)

        @pl.when(m > 0)
        def _():
            mate_copy(m, j).wait()

        return stats(lax.rem(lane + ratio - m, ratio) * heads + i, carry)

    zero = jnp.zeros((8, block), jnp.float32)
    top, total, delta = lax.fori_loop(
        0, members, arrive_turn, (jnp.full((1, block), -1e30, jnp.float32), zero, zero)
    )
    inverse = 1.0 / jnp.sum(total, axis=0, keepdims=True)
    delta = jnp.sum(delta, axis=0, keepdims=True) * inverse
    dq_acc[...] = jnp.zeros_like(dq_acc)

    def terms(slot):
        query = qg_buf[:, 0].reshape(block, HEAD_DIM)
        grad = qg_buf[:, 1].reshape(block, HEAD_DIM)
        weights = z_buf[slot] * (jnp.exp(tops[slot][0:1] - top) * inverse)
        value_term = jnp.dot(
            weights.astype(jnp.bfloat16), grad, preferred_element_type=jnp.float32
        )
        grad_scores = (weights * ((p_buf[slot] - delta) * scaling)).astype(jnp.bfloat16)
        key_term = jnp.dot(grad_scores, query, preferred_element_type=jnp.float32)
        dq_acc[...] += lax.dot_general(
            kv_buf[slot, 0], grad_scores, TN, preferred_element_type=jnp.float32
        )
        return key_term, value_term

    def part_copy(m, i):
        return pltpu.make_async_remote_copy(
            src_ref=part_stage.at[m - 1, i], dst_ref=part_mates.at[m - 1, i],
            send_sem=part_send.at[m, i], recv_sem=part_recv.at[m, i],
            device_id={"seq": mine * ratio + lax.rem(lane + m, ratio), "head": group},
            device_id_type=MESH,
        )

    def back_copy(j):
        i = lax.rem(mine + 1 + j, heads)
        return pltpu.make_async_remote_copy(
            src_ref=kv_final.at[i], dst_ref=kv_back.at[mine],
            send_sem=back_send.at[j], recv_sem=back_recv.at[j],
            device_id={"seq": i * ratio + lane, "head": group}, device_id_type=MESH,
        )

    def mate_part(m, j):
        i = lax.rem(mine + 1 + j, heads)
        key_term, value_term = terms(lax.rem(lane + m, ratio) * heads + i)
        part_stage[m - 1, i, 0] = key_term.astype(jnp.bfloat16)
        part_stage[m - 1, i, 1] = value_term.astype(jnp.bfloat16)
        part_copy(m, i).start()

    def own_part(j):
        i = lax.rem(mine + 1 + j, heads)
        key_term, value_term = terms(lane * heads + i)
        for m in range(1, ratio):
            part_copy(m, i).wait()
            key_term = key_term + part_mates[m - 1, i, 0].astype(jnp.float32)
            value_term = value_term + part_mates[m - 1, i, 1].astype(jnp.float32)
        kv_final[i, 0] = key_term.astype(jnp.bfloat16)
        kv_final[i, 1] = value_term.astype(jnp.bfloat16)

        @pl.when(j < heads - 1)
        def _():
            back_copy(j).start()

    def grads_turn(j, carry):
        @pl.when(j < heads)
        def _():
            def mate_turn(m, inner):
                mate_part(m, j)
                return inner

            lax.fori_loop(1, ratio, mate_turn, 0)

        @pl.when(j > 0)
        def _():
            own_part(j - 1)

        return carry

    lax.fori_loop(0, heads + 1, grads_turn, 0)
    kv_back[mine] = kv_final[mine]

    grad_query = dq_acc[...].T.astype(jnp.bfloat16)
    dq_stage[...] = grad_query.reshape(heads, groups, part_rows, HEAD_DIM)

    def dq_copy(j, e):
        i = lax.rem(mine + 1 + j, heads)
        other = lax.rem(group + e, groups)
        return pltpu.make_async_remote_copy(
            src_ref=dq_stage.at[i, other], dst_ref=dq_back.at[group * heads + mine],
            send_sem=dq_send.at[j, e], recv_sem=dq_recv.at[j, e],
            device_id={"seq": i * ratio + lane, "head": other}, device_id_type=MESH,
        )

    remote = [(j, e) for j in range(heads) for e in range(groups) if (j, e) != (heads - 1, 0)]
    for j, e in remote:
        dq_copy(j, e).start()
    dq_back[group * heads + mine] = dq_stage[mine, group]

    for j in range(heads - 1):
        back_copy(j).wait()
    for h in range(heads):
        dk_out[:, h * HEAD_DIM:(h + 1) * HEAD_DIM] = kv_back[h, 0]
        dv_out[:, h * HEAD_DIM:(h + 1) * HEAD_DIM] = kv_back[h, 1]
    for j, e in remote:
        dq_copy(j, e).wait()
    for h in range(groups * heads):
        dq_out[:, h * HEAD_DIM:(h + 1) * HEAD_DIM] = dq_back[h]


def local(members, groups, query_rows, key_rows, value_rows, grad_output, positions):
    rows, wide = query_rows.shape
    heads = wide // HEAD_DIM
    ratio = members // heads
    width = -(-rows // HEAD_DIM) * HEAD_DIM
    block = heads * rows
    position_rows = jnp.broadcast_to(
        jnp.pad(positions.astype(jnp.float32), (0, width - rows))[None], (8, width)
    )
    low, full = jnp.bfloat16, jnp.float32
    piece = (rows, HEAD_DIM)
    dma = pltpu.SemaphoreType.DMA
    mates = max(ratio - 1, 1)
    scratch = [
        pltpu.VMEM((heads, 2) + piece, low),
        pltpu.VMEM((members, 2) + piece, low),
        pltpu.VMEM((heads, 2) + piece, low),
        pltpu.VMEM((heads, 2) + piece, low),
        pltpu.VMEM((members, 8, width), full),
        pltpu.VMEM((members,) + piece, full),
        pltpu.VMEM((members, 8, block), full),
        pltpu.VMEM((members, rows, block), full),
        pltpu.VMEM((members, rows, block), full),
        pltpu.VMEM((HEAD_DIM, block), full),
        pltpu.VMEM((mates, heads, 2) + piece, low),
        pltpu.VMEM((mates, heads, 2) + piece, low),
        pltpu.VMEM((heads, 2) + piece, low),
        pltpu.VMEM((heads, 2) + piece, low),
        pltpu.VMEM((heads, groups, rows // groups, HEAD_DIM), low),
        pltpu.VMEM((groups * heads, rows // groups, HEAD_DIM), low),
        dma((2, heads)), dma((2, heads)), dma((heads,)), dma((heads,)), dma((heads,)),
        dma((heads,)), dma((members,)), dma((members,)),
        dma((ratio, heads)), dma((ratio, heads)),
        dma((ratio, heads)), dma((ratio, heads)), dma((heads,)), dma((heads,)),
        dma((heads, groups)), dma((heads, groups)),
    ]
    vmem = pl.BlockSpec(memory_space=pltpu.VMEM)
    hbm = pl.BlockSpec(memory_space=pl.ANY)
    return pl.pallas_call(
        functools.partial(kernel, members, heads, groups, rows, width),
        out_shape=(
            jax.ShapeDtypeStruct((rows // groups, groups * wide), low),
            jax.ShapeDtypeStruct((rows, wide), low),
            jax.ShapeDtypeStruct((rows, wide), low),
        ),
        in_specs=[vmem, hbm, hbm, hbm, hbm],
        out_specs=(vmem, vmem, vmem),
        scratch_shapes=scratch,
        compiler_params=pltpu.CompilerParams(
            collective_id=0, has_side_effects=True, vmem_limit_bytes=63 * 1024 * 1024
        ),
    )(position_rows, query_rows, key_rows, value_rows, grad_output)


def solution(mesh):
    placed = (P("seq", "head"), P("seq", "head"), P("seq", "head"), P("seq", "head"), P("seq"))
    return jax.shard_map(
        functools.partial(local, mesh.shape["seq"], mesh.shape["head"]),
        mesh=mesh,
        in_specs=placed,
        out_specs=(P(("seq", "head"), None), P("seq", "head"), P("seq", "head")),
        check_vma=False,
    )
```
